32 devices in a mesh: groups: 1, ep: 16 (over z, y, x), hp: 2 (over core).
Axes of the slice: x: 2, y: 2, z: 4, core: 2. Of those that a mesh axis runs over, the one named last changes fastest.
Arguments:
- x_pre: bfloat16 [896, 1536], P(('groups', 'ep')), may hold values from -6 to 6
- x_dec: bfloat16 [128, 1536], P(('groups', 'ep')), may hold values from -6 to 6
- prefill_query_rows: bfloat16 [896, 2048], P(('groups', 'ep'), 'hp'), may hold values from -240 to 240
- prefill_key_values: bfloat16 [2, 896, 256], P(None, ('groups', 'ep'), 'hp'), may hold values from -6.1 to 6.1
- decode_query_rows: bfloat16 [128, 2048], P(('groups', 'ep'), 'hp'), may hold values from -240 to 240
- decode_key_values: bfloat16 [2, 128, 256], P(None, ('groups', 'ep'), 'hp'), may hold values from -6 to 6
- cache: bfloat16 [2, 128, 128, 256], P(None, ('groups', 'ep'), None, 'hp'), may hold values from -6.1 to 6.1
- cache_len: int32 [128], P(('groups', 'ep')), may hold values from 2 to 128
- sinks: float32 [32], P('hp'), may hold values from -1 to 5
- o_weight: bfloat16 [2048, 1536], P('hp', 'ep'), may hold values from -0.125 to 0.125
- norm_gain: float32 [1536], replicated, may hold values from 0.5 to 1.5
- expert_ids: int32 [1024, 4], P(('groups', 'ep')), may hold values from 0 to 7, all different within a row; in each aligned block of 64 rows (0 to 63, 64 to 127, ...) at most 48 rows name the same one
- route_logits: float32 [1024, 4], P(('groups', 'ep')), may hold values from -6 to 6
- w_gate_up: bfloat16 [16, 2, 1536, 768], P('ep', None, None, 'hp'), may hold values from -0.15625 to 0.15625
- w_down: bfloat16 [16, 768, 1536], P('ep', 'hp'), may hold values from -0.15625 to 0.15625
Outputs:
- layer_out: bfloat16 [1024, 1536], P(('groups', 'ep', 'hp'))
The draws below stay inside these ranges and needn't reach their ends.
Inputs may be any that keep to these rules, and one draw needn't show every extreme that they name: `expert_ids`: each row names 4 different experts; among the rows of one index of ep no expert is named by more than 48 rows, and in every draw some expert is named by exactly 48 rows of some index.
All inputs are finite; a program needn't handle non-finite values.
Results may differ from the reference program's by a relative error of at most 0.0065.
Values may be sent and summed in bfloat16 or wider, within the bound.
A program may use at most 64 MiB of HBM per device.

```python
import math
import jax
import jax.numpy as jnp
import numpy as np
from jax import lax

D = 1536
QUERY_HEADS = 32
LOCAL_KV_HEADS = 4
HEAD_SIZE = 64
FF = 1536
TOPK = 4
PREFILL_LOCAL = 56
DEC_DEV = 8
CACHE_POSITIONS = 128
EXPERTS = 8
PREFILL_TOKENS = 896
DECODE_COUNT = 128
TOK_DEV = 64
TOKENS = 1024
SLOT = 48
N_EP = 16


def prefill_index_pairs(key):
    base_offset = jax.random.normal(jax.random.fold_in(key, 11), (2, PREFILL_TOKENS, LOCAL_KV_HEADS * HEAD_SIZE), jnp.float32)
    return jnp.clip(base_offset, -6.1, 6.1)


def draw_prefill_key_values(key, part):
    return prefill_index_pairs(key).astype(jnp.bfloat16)


def draw_prefill_query_rows(key, part):
    base_offset = jnp.clip(jax.random.normal(jax.random.fold_in(key, 13), (PREFILL_TOKENS, QUERY_HEADS * HEAD_SIZE), jnp.float32), -6.0, 6.0)
    return jnp.clip(base_offset, -240.0, 240.0).astype(jnp.bfloat16)


def draw_cache(key, part):
    base_offset = jnp.clip(jax.random.normal(jax.random.fold_in(key, 22), (2, DECODE_COUNT, CACHE_POSITIONS, LOCAL_KV_HEADS * HEAD_SIZE), jnp.float32), -6.0, 6.0)
    return base_offset.astype(jnp.bfloat16)


def draw_decode_query_rows(key, part):
    base_offset = jnp.clip(jax.random.normal(jax.random.fold_in(key, 23), (DECODE_COUNT, QUERY_HEADS * HEAD_SIZE), jnp.float32), -6.0, 6.0)
    return jnp.clip(base_offset, -240.0, 240.0).astype(jnp.bfloat16)


def plant(values, key, smallest, top_value):
    shape = values.shape
    index_at = [jax.random.randint(jax.random.fold_in(key, axis), (), 0, shape[axis]) for axis in range(len(shape))]
    values = values.at[tuple(index_at)].set(smallest)
    longest = shape.index(max(shape))
    index_at[longest] = (index_at[longest] + 1) % shape[longest]
    return values.at[tuple(index_at)].set(top_value)


def shard_levels(stream_key, dims, pieces, least, largest):
    factor_of, own = 1.0, jax.random.fold_in(stream_key, 6)
    for axis_at, parts in pieces:
        draws = jnp.exp(jax.random.uniform(jax.random.fold_in(own, axis_at), (parts,), jnp.float32, least / len(pieces), largest / len(pieces)))
        factor_of = factor_of * jnp.repeat(draws, dims[axis_at] // parts).reshape([-1 if axis == axis_at else 1 for axis in range(len(dims))])
    return factor_of


def shared_out(key, own, number, rows, number_of, top, limit, lean):
    ranking = jax.random.permutation(key, number_of)
    heavy_load, ordinary = portions_of(number_of, rows * top, limit, lean, True), portions_of(number_of, rows * top, limit, lean, False)
    places = jnp.arange(number_of)

    def named(sizes, offset_by):
        used = int((sizes > 0).sum())
        fixed = max(1, used // 4)
        shifted = fixed + (places - fixed + offset_by * (used - fixed)) % max(1, number_of - fixed)
        return jnp.zeros((number_of,), jnp.int32).at[ranking[jnp.where(places < fixed, places, shifted)]].set(jnp.asarray(sizes, jnp.int32))

    sizes = jnp.where(number % 4 == 0, named(heavy_load, number // 4), named(ordinary, number - number // 4 - 1))
    mixed = jax.random.permutation(jax.random.fold_in(own, 3), number_of)
    giver, receiver = mixed[0:number_of // 2 * 2:2], mixed[1:number_of // 2 * 2:2]
    room = jnp.minimum(sizes[giver] - 1, limit - sizes[receiver]) // 2
    room = jnp.where((giver == ranking[0]) | (receiver == ranking[0]) | (sizes[receiver] == 0), 0, jnp.maximum(room, 0))
    shifted = jax.random.randint(jax.random.fold_in(own, 4), (number_of // 2,), 0, 1 << 20) % (room + 1)
    sizes = sizes.at[giver].add(-shifted).at[receiver].add(shifted)
    items = jnp.searchsorted(jnp.cumsum(sizes), jnp.arange(rows * top), side="right").astype(jnp.int32)
    grid = items.reshape(top, rows).T
    grid = grid[jax.random.permutation(jax.random.fold_in(own, 1), rows)]
    offset_by = jax.random.randint(jax.random.fold_in(own, 2), (rows, 1), 0, top)
    return jnp.take_along_axis(grid, (jnp.arange(top)[None, :] + offset_by) % top, axis=1)


def portions_of(number_of, total, most, skew, full):
    weights = [(1 << 20) // math.isqrt(rank ** skew) + 1 for rank in range(1, number_of + 1)]
    largest = most if full else min(most, max(-(-total // number_of), total * weights[0] // sum(weights)))
    least = 1 if total - largest >= number_of - 1 else 0
    given, spare = [largest] + [least] * (number_of - 1), total - largest - least * (number_of - 1)
    while spare > 0:
        candidates = [i for i in range(1, number_of) if given[i] < largest] or [i for i in range(1, number_of) if given[i] < most]
        whole, budget = sum([weights[i] for i in candidates]), spare
        for i in candidates:
            extra = min(most - given[i], max(1, budget * weights[i] // whole), spare)
            given[i] = given[i] + extra
            spare = spare - extra
    return np.array(given)


def centred(stream_key, extent, deviation, limit, split=(), held_as=jnp.bfloat16):
    array = deviation * jax.random.normal(stream_key, extent, jnp.float32)
    if split:
        array = array * shard_levels(stream_key, extent, split, -0.22, 0.18)
    return jnp.clip(array, -limit, limit).astype(held_as)


def setup_inputs(seed: int = 0, part: int = 0) -> dict:
    streams_of = jax.random.split(jax.random.key(seed), 16)
    part_keys = jax.random.split(jax.random.fold_in(streams_of[15], part), 16)
    x_pre = centred(part_keys[0], (PREFILL_TOKENS, D), 1.0, 6.0, ((0, 16),))
    x_dec = centred(part_keys[1], (DECODE_COUNT, D), 1.0, 6.0, ((0, 16),))
    prefill_query_rows = draw_prefill_query_rows(jax.random.fold_in(jax.random.fold_in(streams_of[15], part), 71), part)
    prefill_key_values = draw_prefill_key_values(jax.random.fold_in(jax.random.fold_in(streams_of[15], part), 71), part)
    decode_query_rows = draw_decode_query_rows(jax.random.fold_in(jax.random.fold_in(streams_of[15], part), 71), part)
    decode_key_values = centred(part_keys[5], (2, DECODE_COUNT, LOCAL_KV_HEADS * HEAD_SIZE), 1.0, 6.0, ((1, 16), (2, 2)))
    cache = draw_cache(jax.random.fold_in(jax.random.fold_in(streams_of[15], part), 71), part)
    cache_len = plant(jax.random.randint(part_keys[7], (DECODE_COUNT,), 2, CACHE_POSITIONS + 1), jax.random.fold_in(part_keys[7], 1), 2, CACHE_POSITIONS).astype(jnp.int32)
    sinks = jnp.clip(-1.0 + 6.0 * jax.random.uniform(streams_of[8], (QUERY_HEADS,), jnp.float32) ** shard_levels(streams_of[8], (QUERY_HEADS,), ((0, 2),), -0.2, 0.2), -1.0, 5.0)
    o_weight = centred(streams_of[9], (QUERY_HEADS * HEAD_SIZE, D), (QUERY_HEADS * HEAD_SIZE) ** -0.5, 0.125, ((0, 2), (1, 16)))
    norm_gain = jnp.clip(1.0 + 0.1 * jax.random.normal(streams_of[10], (D,), jnp.float32), 0.5, 1.5)
    expert_ids_keys = jax.random.split(jax.random.fold_in(part_keys[11], 1), TOKENS // TOK_DEV)
    expert_ids_turns = jax.random.permutation(jax.random.fold_in(part_keys[11], 3), TOKENS // TOK_DEV)
    expert_ids = jax.vmap(lambda own, number: shared_out(jax.random.fold_in(part_keys[11], 2), own, number, TOK_DEV, EXPERTS, TOPK, SLOT, 2))(expert_ids_keys, expert_ids_turns).reshape((TOKENS, TOPK))
    route_logits = centred(part_keys[12], (TOKENS, TOPK), 1.5, 6.0, ((0, 16),), jnp.float32)
    w_gate_up = centred(streams_of[13], (2 * EXPERTS, 2, D, FF // 2), D ** -0.5, 0.15625, ((0, 16), (3, 2)))
    w_down = centred(streams_of[14], (2 * EXPERTS, FF // 2, D), FF ** -0.5, 0.15625, ((0, 16), (1, 2)))
    return {"x_pre": x_pre, "x_dec": x_dec, "prefill_query_rows": prefill_query_rows, "prefill_key_values": prefill_key_values, "decode_query_rows": decode_query_rows, "decode_key_values": decode_key_values, "cache": cache, "cache_len": cache_len, "sinks": sinks, "o_weight": o_weight, "norm_gain": norm_gain, "expert_ids": expert_ids, "route_logits": route_logits, "w_gate_up": w_gate_up, "w_down": w_down}


EPS = 1e-05

def softmax_probability(scores, sink_logit_bias):
    top = jnp.maximum(lax.optimization_barrier(jnp.max(scores, axis=-1, keepdims=True)), sink_logit_bias)
    expo = jnp.exp(scores - top)
    total = lax.optimization_barrier(jnp.sum(expo, axis=-1, keepdims=True)) + jnp.exp(sink_logit_bias - top)
    return (expo / total).astype(jnp.bfloat16)

def prefill_attention(prefill_query_rows, prefill_key_values, sinks):
    head_group = QUERY_HEADS // LOCAL_KV_HEADS
    block_list = PREFILL_TOKENS // PREFILL_LOCAL
    key_rows = prefill_key_values[0].reshape(block_list, PREFILL_LOCAL, LOCAL_KV_HEADS, HEAD_SIZE)
    value_rows = prefill_key_values[1].reshape(block_list, PREFILL_LOCAL, LOCAL_KV_HEADS, HEAD_SIZE)
    query_rows = prefill_query_rows.reshape(block_list, PREFILL_LOCAL, LOCAL_KV_HEADS, head_group, HEAD_SIZE)
    sink_logit_bias = sinks.reshape(LOCAL_KV_HEADS, head_group)[None, :, :, None]
    places = jnp.arange(PREFILL_LOCAL, dtype=jnp.int32)
    visible = places[None, :] <= places[:, None]

    def one_block(args):
        rows, block_keys, block_values = args
        scores = jnp.einsum('qhgd,khd->qhgk', rows.astype(jnp.float32), block_keys.astype(jnp.float32)) * HEAD_SIZE ** (-0.5)
        scores = jnp.where(visible[:, None, None, :], scores, -jnp.inf)
        weight_matrix = softmax_probability(scores, sink_logit_bias)
        out = jnp.einsum('qhgk,khd->qhgd', weight_matrix.astype(jnp.float32), block_values.astype(jnp.float32))
        return out.astype(jnp.bfloat16).reshape(PREFILL_LOCAL, QUERY_HEADS * HEAD_SIZE)
    return lax.map(one_block, (query_rows, key_rows, value_rows)).reshape(PREFILL_TOKENS, QUERY_HEADS * HEAD_SIZE)

def decode_attention(decode_query_rows, decode_key_values, cache, cache_len, sinks):
    head_group = QUERY_HEADS // LOCAL_KV_HEADS
    query_rows = decode_query_rows.reshape(DECODE_COUNT, LOCAL_KV_HEADS, head_group, HEAD_SIZE).astype(jnp.float32)
    cached_key_rows = cache[0].reshape(DECODE_COUNT, CACHE_POSITIONS, LOCAL_KV_HEADS, HEAD_SIZE).astype(jnp.float32)
    cached_value_rows = cache[1].reshape(DECODE_COUNT, CACHE_POSITIONS, LOCAL_KV_HEADS, HEAD_SIZE).astype(jnp.float32)
    own_key_rows = decode_key_values[0].reshape(DECODE_COUNT, LOCAL_KV_HEADS, HEAD_SIZE).astype(jnp.float32)
    own_value_rows = decode_key_values[1].reshape(DECODE_COUNT, LOCAL_KV_HEADS, HEAD_SIZE).astype(jnp.float32)
    past_positions = jnp.einsum('shgd,sjhd->shgj', query_rows, cached_key_rows) * HEAD_SIZE ** (-0.5)
    live = jnp.arange(CACHE_POSITIONS, dtype=jnp.int32)[None, :] < cache_len[:, None]
    past_positions = jnp.where(live[:, None, None, :], past_positions, -jnp.inf)
    own_token = jnp.einsum('shgd,shd->shg', query_rows, own_key_rows)[..., None] * HEAD_SIZE ** (-0.5)
    weight_matrix = softmax_probability(jnp.concatenate([past_positions, own_token], axis=-1), sinks.reshape(LOCAL_KV_HEADS, head_group)[None, :, :, None])
    weight_matrix = weight_matrix.astype(jnp.float32)
    out = jnp.einsum('shgj,sjhd->shgd', weight_matrix[..., :CACHE_POSITIONS], cached_value_rows)
    out = out + weight_matrix[..., CACHE_POSITIONS:] * own_value_rows[:, :, None, :]
    return out.astype(jnp.bfloat16).reshape(DECODE_COUNT, QUERY_HEADS * HEAD_SIZE)

def device_major(pre, dec):
    first = pre.reshape(N_EP, PREFILL_LOCAL, pre.shape[-1])
    second = dec.reshape(N_EP, DEC_DEV, dec.shape[-1])
    return jnp.concatenate([first, second], axis=1).reshape(N_EP * (PREFILL_LOCAL + DEC_DEV), pre.shape[-1])

def reference(x_pre, x_dec, prefill_query_rows, prefill_key_values, decode_query_rows, decode_key_values, cache, cache_len, sinks, o_weight, norm_gain, expert_ids, route_logits, w_gate_up, w_down):
    attended = device_major(prefill_attention(prefill_query_rows, prefill_key_values, sinks), decode_attention(decode_query_rows, decode_key_values, cache, cache_len, sinks))
    stream = device_major(x_pre, x_dec).astype(jnp.float32) + jnp.dot(attended, o_weight, preferred_element_type=jnp.float32)
    mean_sq = lax.optimization_barrier(jnp.mean(stream * stream, axis=-1, keepdims=True))
    normed = (stream * lax.rsqrt(mean_sq + EPS) * norm_gain).astype(jnp.bfloat16)
    flat_ids = expert_ids.reshape(-1)
    capacity = N_EP * SLOT
    quarter = FF // 4

    def one_holder(outputs, args):
        expert, gate_up, down = args
        chosen = flat_ids == expert
        picked = jnp.nonzero(chosen, size=capacity, fill_value=0)[0].astype(jnp.int32)
        count = jnp.sum(chosen.astype(jnp.int32))
        live = (jnp.arange(capacity, dtype=jnp.int32) < count).astype(jnp.float32)
        rows = normed[picked // TOPK]
        gate = jnp.dot(rows, gate_up[0], preferred_element_type=jnp.float32)
        upper = jnp.dot(rows, gate_up[1], preferred_element_type=jnp.float32)
        hidden = ((upper + 1.0) * gate * jax.nn.sigmoid(1.702 * gate)).astype(jnp.bfloat16)
        lower_part = jnp.dot(hidden[:, :quarter], down[:quarter], preferred_element_type=jnp.float32).astype(jnp.bfloat16)
        upper_part = jnp.dot(hidden[:, quarter:], down[quarter:], preferred_element_type=jnp.float32).astype(jnp.bfloat16)
        lower_part, upper_part = lax.optimization_barrier((lower_part, upper_part))
        result = (lower_part.astype(jnp.float32) + upper_part.astype(jnp.float32)).astype(jnp.bfloat16)
        result = lax.optimization_barrier(result).astype(jnp.float32) * live[:, None]
        return (outputs.at[picked].add(result), None)
    holders = jnp.arange(2 * EXPERTS, dtype=jnp.int32) // 2
    outputs, _ = lax.scan(one_holder, jnp.zeros((TOKENS * TOPK, D), jnp.float32), (holders, w_gate_up, w_down))
    mix = jax.nn.softmax(route_logits, axis=-1)
    moe = lax.optimization_barrier(jnp.sum(outputs.reshape(TOKENS, TOPK, D) * mix[:, :, None], axis=1))
    return (stream + moe).astype(jnp.bfloat16)
```

```python
import functools

import jax
import jax.numpy as jnp
from jax import lax
from jax.experimental import pallas as pl
from jax.experimental.pallas import tpu as pltpu
from jax.sharding import PartitionSpec as P

HEAD_SIZE = 64


EPS = 1e-05


def softmax_probability(scores, sink_logit_bias):
    top = jnp.maximum(jnp.max(scores, axis=-1, keepdims=True), sink_logit_bias)
    expo = jnp.exp(scores - top)
    total = jnp.sum(expo, axis=-1, keepdims=True) + jnp.exp(sink_logit_bias - top)
    return (expo / total).astype(jnp.bfloat16)


def rms_norm(stream, gain):
    mean_sq = jnp.mean(stream * stream, axis=-1, keepdims=True)
    return (stream * lax.rsqrt(mean_sq + EPS) * gain).astype(jnp.bfloat16)


def attention_rows(
    x_pre,
    x_dec,
    prefill_query_rows,
    prefill_key_values,
    decode_query_rows,
    decode_key_values,
    cache,
    cache_len,
    sinks):
    pre_rows, width = x_pre.shape
    dec_rows = x_dec.shape[0]
    kv_heads = prefill_key_values.shape[2] // HEAD_SIZE
    q_heads = sinks.shape[0]
    head_group = q_heads // kv_heads
    kv_max = cache.shape[2]
    scale = HEAD_SIZE ** (-0.5)
    sink_logit_bias = sinks.reshape(kv_heads, head_group)[None, :, :, None]
    keys_here = prefill_key_values[0].reshape(pre_rows, kv_heads, HEAD_SIZE)
    values_here = prefill_key_values[1].reshape(pre_rows, kv_heads, HEAD_SIZE)
    query_rows = prefill_query_rows.reshape(pre_rows, kv_heads, head_group, HEAD_SIZE)
    scores = (
        jnp.einsum("qhgd,khd->qhgk", query_rows, keys_here, preferred_element_type=jnp.float32)
        * scale
    )
    places = jnp.arange(pre_rows, dtype=jnp.int32)
    visible = places[None, :] <= places[:, None]
    scores = jnp.where(visible[:, None, None, :], scores, -jnp.inf)
    weight_matrix = softmax_probability(scores, sink_logit_bias)
    pre_out = jnp.einsum(
        "qhgk,khd->qhgd", weight_matrix, values_here, preferred_element_type=jnp.float32
    )
    pre_out = pre_out.astype(jnp.bfloat16).reshape(pre_rows, q_heads * HEAD_SIZE)
    dec_queries = decode_query_rows.reshape(dec_rows, kv_heads, head_group, HEAD_SIZE)
    cached_key_rows = cache[0].reshape(dec_rows, kv_max, kv_heads, HEAD_SIZE)
    cached_value_rows = cache[1].reshape(dec_rows, kv_max, kv_heads, HEAD_SIZE)
    own_key_rows = decode_key_values[0].reshape(dec_rows, kv_heads, HEAD_SIZE)
    own_value_rows = decode_key_values[1].reshape(dec_rows, kv_heads, HEAD_SIZE)
    past_positions = (
        jnp.einsum(
            "shgd,sjhd->shgj", dec_queries, cached_key_rows, preferred_element_type=jnp.float32
        )
        * scale
    )
    live = jnp.arange(kv_max, dtype=jnp.int32)[None, :] < cache_len[:, None]
    past_positions = jnp.where(live[:, None, None, :], past_positions, -jnp.inf)
    own_token = (
        jnp.einsum("shgd,shd->shg", dec_queries, own_key_rows, preferred_element_type=jnp.float32)[
            ..., None
        ]
        * scale
    )
    dec_weights = softmax_probability(
        jnp.concatenate([past_positions, own_token], axis=-1), sink_logit_bias
    )
    dec_out = jnp.einsum(
        "shgj,sjhd->shgd",
        dec_weights[..., :kv_max],
        cached_value_rows,
        preferred_element_type=jnp.float32,
    )
    dec_out = (
        dec_out
        + dec_weights[..., kv_max:].astype(jnp.float32)
        * own_value_rows.astype(jnp.float32)[:, :, None, :]
    )
    dec_out = dec_out.astype(jnp.bfloat16).reshape(dec_rows, q_heads * HEAD_SIZE)
    attn_rows = jnp.concatenate([pre_out, dec_out], axis=0)
    return attn_rows
def general_path(
    x_pre,
    x_dec,
    prefill_query_rows,
    prefill_key_values,
    decode_query_rows,
    decode_key_values,
    cache,
    cache_len,
    sinks,
    o_weight,
    norm_gain,
    expert_ids,
    route_logits,
    w_gate_up,
    w_down,
):
    attn_rows = attention_rows(
        x_pre,
        x_dec,
        prefill_query_rows,
        prefill_key_values,
        decode_query_rows,
        decode_key_values,
        cache,
        cache_len,
        sinks,
    )
    width = x_pre.shape[1]
    resid = jnp.concatenate([x_pre, x_dec], axis=0).astype(jnp.float32)
    half = attn_rows.shape[0] // 2
    mine = lax.axis_index("hp") * half
    head_part = jnp.dot(
        attn_rows,
        lax.all_gather(o_weight, "ep", axis=1, tiled=True),
        preferred_element_type=jnp.float32,
    )
    summed = lax.psum_scatter(head_part, "hp", scatter_dimension=0, tiled=True)
    stream = lax.dynamic_slice_in_dim(resid, mine, half, 0) + summed
    normed = lax.all_gather(rms_norm(stream, norm_gain), "hp", axis=0, tiled=True)
    tokens_here, topk = expert_ids.shape
    holders = lax.axis_size("ep")
    experts = holders // 2
    slot = min(
        tokens_here, 2 * ((3 * max(1, (tokens_here * topk + experts - 1) // experts) + 3) // 4)
    )
    plane = slot // 2
    flat_ids = expert_ids.reshape(-1)
    onehot = (flat_ids[:, None] == jnp.arange(experts, dtype=jnp.int32)[None, :]).astype(jnp.int32)
    rank = jnp.sum(jnp.cumsum(onehot, axis=0) * onehot, axis=1) - 1
    position = (flat_ids * slot + rank).reshape(tokens_here, topk)
    columns = jnp.arange(experts * slot, dtype=jnp.int32)[None, None, :] == position[:, :, None]
    picked_rows = jnp.any(columns, axis=1).T.astype(jnp.bfloat16)
    per_expert = (
        jnp.dot(picked_rows, normed, preferred_element_type=jnp.float32)
        .astype(jnp.bfloat16)
        .reshape(experts, slot, width)
    )
    send = jnp.repeat(per_expert, 2, axis=0)
    own_plane = lax.dynamic_slice_in_dim(send, lax.axis_index("hp") * plane, plane, 1)
    arrived_plane = lax.all_to_all(own_plane, "ep", split_axis=0, concat_axis=0, tiled=True)
    arrived = lax.all_gather(arrived_plane, "hp", axis=1, tiled=True)
    rows = arrived.reshape(-1, width)
    gate = jnp.dot(rows, w_gate_up[0, 0], preferred_element_type=jnp.float32)
    upper = jnp.dot(rows, w_gate_up[0, 1], preferred_element_type=jnp.float32)
    hidden = ((upper + 1.0) * gate * jax.nn.sigmoid(1.702 * gate)).astype(jnp.bfloat16)
    partial_out = jnp.dot(hidden, w_down[0], preferred_element_type=jnp.float32).reshape(
        -1, slot, width
    )
    share = lax.psum_scatter(
        partial_out.astype(jnp.bfloat16), "hp", scatter_dimension=1, tiled=True
    )
    returned = lax.all_to_all(share, "ep", split_axis=0, concat_axis=0, tiled=True)
    mix = jax.nn.softmax(route_logits, axis=-1)
    blend = jnp.sum(jnp.where(columns, mix[:, :, None], 0.0), axis=1).reshape(
        tokens_here, experts, slot
    )
    blend = jnp.repeat(blend, 2, axis=1)
    blend_plane = lax.dynamic_slice_in_dim(blend, lax.axis_index("hp") * plane, plane, 2).reshape(
        tokens_here, holders * plane
    )
    terms = jnp.dot(
        blend_plane,
        returned.reshape(-1, width).astype(jnp.float32),
        precision=lax.Precision.HIGHEST,
    )
    moe = lax.psum_scatter(
        terms.astype(jnp.bfloat16), "hp", scatter_dimension=0, tiled=True
    ).astype(jnp.float32)
    return (stream + moe).astype(jnp.bfloat16)


MESH = pl.DeviceIdType.MESH
LANES = 128
NT = (((1,), (1,)), ((), ()))


def f32_dot(a, b):
    return jnp.dot(a, b, preferred_element_type=jnp.float32)


def f32_dot_nt(a, b):
    return lax.dot_general(a, b, NT, preferred_element_type=jnp.float32)


def layer_kernel(
    xp_hbm,
    xd_hbm,
    qp_hbm,
    kvp_hbm,
    qd_hbm,
    kvd_hbm,
    cache_hbm,
    lens_hbm,
    sinks_hbm,
    wo_hbm,
    gain_hbm,
    ids_hbm,
    logits_hbm,
    gu_hbm,
    dn_hbm,
    out_ref,
    xp,
    xd,
    qp,
    kvp,
    qd,
    kvd,
    cache,
    lens,
    sinks,
    gain,
    ids,
    logits,
    gu,
    dn,
    wo_all,
    mix_all,
    mix_cols,
    attn_all,
    proj,
    proj_in,
    ret,
    columns,
    kept_rows,
    tok,
    part_out,
    from_core,
    from_first,
    mid,
    from_second,
    to_send,
    from_z,
    send_sem,
    recv_sem,
    load_sem,
):
    me = lax.axis_index("ep")
    core = lax.axis_index("hp")
    x, y, z = lax.rem(me, 2), lax.rem(me // 2, 2), me // 4
    zl, zh = lax.rem(z, 2), z // 2
    other = 1 - core
    zk = [z, zh * 2 + 1 - zl, (1 - zh) * 2 + zl, (1 - zh) * 2 + 1 - zl]
    to_x = {"ep": z * 4 + y * 2 + (1 - x)}
    to_y = {"ep": z * 4 + (1 - y) * 2 + x}
    to_z = [None] + [{"ep": zk[k] * 4 + y * 2 + x} for k in range(1, 4)]
    to_core = {"hp": other}

    loads = []

    def load(source, target):
        copy = pltpu.make_async_copy(source, target, load_sem.at[len(loads)])
        copy.start()
        loads.append(copy)
        return copy

    load_wo = load(wo_hbm, wo_all.at[y, x])
    load_lens = load(lens_hbm, lens)
    load_sinks = load(sinks_hbm, sinks)
    load_qp = load(qp_hbm, qp)
    load_kvp = load(kvp_hbm, kvp)
    load_qd = load(qd_hbm, qd)
    load_kvd = load(kvd_hbm, kvd)
    load_cache = load(cache_hbm, cache)
    load_ids = load(ids_hbm, ids)
    load_logits = load(logits_hbm, logits)
    load_xp = load(xp_hbm, xp)
    load_xd = load(xd_hbm, xd)
    load_gain = load(gain_hbm, gain)
    load_gu = load(gu_hbm, gu)
    load_dn = load(dn_hbm, dn)

    barrier = pltpu.get_barrier_semaphore()
    partners = [to_x, to_y, to_core] + to_z[1:]
    for partner in partners:
        pl.semaphore_signal(barrier, inc=1, device_id=partner, device_id_type=MESH)
    pl.semaphore_wait(barrier, len(partners))

    sent = []

    def push(source, target, device):
        i = len(sent)
        copy = pltpu.make_async_remote_copy(
            src_ref=source,
            dst_ref=target,
            send_sem=send_sem.at[i],
            recv_sem=recv_sem.at[i],
            device_id=device,
            device_id_type=MESH,
        )
        copy.start()
        sent.append(copy)
        return copy

    def send(block, device):
        return push(block, block, device)

    bf = jnp.bfloat16
    f32 = jnp.float32

    load_wo.wait()
    cols = wo_all.shape[2]
    piece = cols // 2
    wo_part = lambda yy, xx, p: wo_all.at[yy, xx, pl.ds(p * piece, piece)]
    wo_first = [send(wo_part(y, x, 0), to_y), send(wo_part(y, x, 1), to_x)]
    wo_last = [send(wo_part(y, x, 0), to_x), send(wo_part(y, x, 1), to_y)]

    tokens = logits.shape[1]
    experts = mix_all.shape[4]
    load_ids.wait()
    load_logits.wait()
    scores = logits[...]
    raised = jnp.exp(scores - jnp.max(scores, axis=0, keepdims=True))
    mix = raised / jnp.sum(raised, axis=0, keepdims=True)
    named = ids[...]
    expert_row = lax.broadcasted_iota(jnp.int32, (experts, tokens), 0)
    blend = jnp.zeros((experts, tokens), f32)
    for k in range(named.shape[0]):
        blend = blend + jnp.where(expert_row == named[k : k + 1], mix[k : k + 1], 0.0)
    spare = mix_all.shape[5] - tokens
    if spare:
        blend = jnp.concatenate([blend, jnp.zeros((experts, spare), f32)], axis=1)
    mix_all[zh, zl, y, x] = blend
    mix_copy = send(mix_all.at[zh, zl, y, x], to_x)

    scale = HEAD_SIZE ** (-0.5)
    kv_heads = kvp.shape[2] // HEAD_SIZE
    pre = qp.shape[0]
    dec = qd.shape[0]
    inner = qp.shape[1]
    pairs = inner // LANES
    per_kv = pairs // kv_heads
    low1 = lax.broadcasted_iota(jnp.int32, (1, LANES), 1) < HEAD_SIZE
    for copy in (load_lens, load_sinks, load_qp, load_kvp, load_qd, load_kvd):
        copy.wait()

    def half_lanes(shape):
        return lax.broadcasted_iota(jnp.int32, shape, len(shape) - 1) < HEAD_SIZE

    def doubled(rows, j):
        turned = pltpu.roll(rows, HEAD_SIZE, 1)
        low = half_lanes(rows.shape)
        even, odd = (rows, turned) if j == 0 else (turned, rows)
        gap = jnp.zeros((HEAD_SIZE - pre, LANES), f32)
        stack = [jnp.where(low, even, 0.0)]
        if HEAD_SIZE > pre:
            stack.append(gap)
        stack.append(jnp.where(low, 0.0, odd))
        if HEAD_SIZE > pre:
            stack.append(gap)
        return jnp.concatenate(stack, axis=0).astype(bf)

    def prefill(j):
        keys = doubled(kvp[0].astype(f32), j)
        values = doubled(kvp[1].astype(f32), j)
        queries = jnp.concatenate(
            [
                qp[:, i * LANES : (i + 1) * LANES].astype(f32)
                for i in range(j * per_kv, (j + 1) * per_kv)
            ],
            axis=0,
        ).astype(bf)
        products = f32_dot_nt(queries, keys) * scale
        shape = (pre, LANES)
        low = half_lanes(shape)
        key_at = lax.broadcasted_iota(jnp.int32, shape, 1)
        key_at = jnp.where(low, key_at, key_at - HEAD_SIZE)
        seen = key_at <= lax.broadcasted_iota(jnp.int32, shape, 0)
        weights = []
        for n in range(per_kv):
            head = 2 * (j * per_kv + n)
            sink_even, sink_odd = sinks[head], sinks[head + 1]
            s = jnp.where(seen, products[n * pre : (n + 1) * pre], -jnp.inf)
            top_even = jnp.max(jnp.where(low, s, -jnp.inf), axis=1, keepdims=True)
            top_odd = jnp.max(jnp.where(low, -jnp.inf, s), axis=1, keepdims=True)
            top_even = jnp.maximum(top_even, sink_even)
            top_odd = jnp.maximum(top_odd, sink_odd)
            expo = jnp.exp(s - jnp.where(low, top_even, top_odd))
            sum_even = jnp.sum(jnp.where(low, expo, 0.0), axis=1, keepdims=True)
            sum_odd = jnp.sum(jnp.where(low, 0.0, expo), axis=1, keepdims=True)
            sum_even = sum_even + jnp.exp(sink_even - top_even)
            sum_odd = sum_odd + jnp.exp(sink_odd - top_odd)
            weights.append(expo / jnp.where(low, sum_even, sum_odd))
        weights = jnp.concatenate(weights, axis=0).astype(bf)
        return f32_dot(weights, values)

    def decode():
        kv_max = cache.shape[2]
        lane = half_lanes((dec, LANES))
        even, odd = [], []
        for i in range(pairs):
            block = qd[:, i * LANES : (i + 1) * LANES].astype(f32)
            turned = pltpu.roll(block, HEAD_SIZE, 1)
            if i < per_kv:
                even.append(jnp.where(lane, block, 0.0))
                odd.append(jnp.where(lane, turned, 0.0))
            else:
                even.append(jnp.where(lane, 0.0, turned))
                odd.append(jnp.where(lane, 0.0, block))
        queries = jnp.concatenate(even + odd, axis=0)
        rows = queries.shape[0]
        groups = rows // dec
        row_seq = lax.rem(lax.broadcasted_iota(jnp.int32, (rows, LANES), 0), dec)
        load_cache.wait()
        products = jnp.zeros((rows, kv_max), f32)
        for s in range(dec):
            mine = jnp.where(row_seq == s, queries, 0.0).astype(bf)
            products = products + f32_dot_nt(mine, cache[0, s])
        grouped = (groups, dec, kv_max)
        products = products.reshape(grouped) * scale
        seq = lax.broadcasted_iota(jnp.int32, (dec, kv_max), 0)
        limit = jnp.zeros((dec, kv_max), jnp.int32)
        for s in range(dec):
            limit = jnp.where(seq == s, lens[s], limit)
        live = lax.broadcasted_iota(jnp.int32, (dec, kv_max), 1) < limit
        products = jnp.where(live[None], products, -jnp.inf)
        own_key = kvd[0].astype(f32)
        own_value = kvd[1].astype(f32)
        own = jnp.sum(queries.reshape(groups, dec, LANES) * own_key[None], axis=2, keepdims=True)
        own = own * scale
        sink = jnp.concatenate(
            [jnp.full((1, dec, 1), sinks[2 * i + odd_head], f32) for odd_head in range(2) for i in range(pairs)],
            axis=0,
        )
        top = jnp.maximum(jnp.max(products, axis=2, keepdims=True), own)
        top = jnp.maximum(top, sink)
        expo = jnp.exp(products - top)
        own_expo = jnp.exp(own - top)
        total = jnp.sum(expo, axis=2, keepdims=True) + own_expo + jnp.exp(sink - top)
        weights = (expo / total).reshape(rows, kv_max)
        own_weight = (own_expo / total).astype(bf).astype(f32)
        summed = jnp.zeros((rows, LANES), f32)
        row_seq = lax.rem(lax.broadcasted_iota(jnp.int32, (rows, kv_max), 0), dec)
        for s in range(dec):
            mine = jnp.where(row_seq == s, weights, 0.0).astype(bf)
            summed = summed + f32_dot(mine, cache[1, s])
        summed = summed.reshape(groups, dec, LANES) + own_weight * own_value[None]
        out = []
        for i in range(pairs):
            a, b = summed[i], summed[pairs + i]
            if i < per_kv:
                out.append(jnp.where(lane, a, pltpu.roll(b, HEAD_SIZE, 1)))
            else:
                out.append(jnp.where(lane, pltpu.roll(a, HEAD_SIZE, 1), b))
        return out

    def keep_attention(j, pre_out, dec_out):
        for n in range(per_kv):
            block = jnp.concatenate(
                [pre_out[n * pre : (n + 1) * pre], dec_out[j * per_kv + n]], axis=0
            )
            attn_all[0, j, :, n * LANES : (n + 1) * LANES] = block.astype(bf)

    heads = [None, [], [], []]

    def send_attention(j):
        heads[2].append(push(attn_all.at[0, j], attn_all.at[2, j], to_z[2]))
        heads[1].append(push(attn_all.at[0, j], attn_all.at[1, j], to_z[1]))

    pre_out = prefill(0)
    dec_out = decode()
    keep_attention(0, pre_out, dec_out)
    send_attention(0)
    for j in range(1, kv_heads):
        keep_attention(j, prefill(j), dec_out)
        send_attention(j)

    mix_copy.wait_recv()
    mix_copy = send(mix_all.at[zh, zl, y], to_y)
    wo_first[0].wait_recv()
    wo_last.append(send(wo_part(1 - y, x, 0), to_x))
    wo_first[1].wait_recv()
    wo_last.append(send(wo_part(y, 1 - x, 1), to_y))
    mix_copy.wait_recv()
    mix_copy = send(mix_all.at[zh, zl], to_z[1])
    heads[2][0].wait_recv()
    heads[3].append(push(attn_all.at[2, 0], attn_all.at[3, 0], to_z[1]))
    for copy in wo_last:
        copy.wait_recv()

    half = tokens // 2
    width = xp.shape[1]
    part = inner // kv_heads

    exchange = []

    def project(k):
        total = 0.0
        for j in range(kv_heads):
            weight = wo_all[:, :, :, j * part : (j + 1) * part].reshape(4 * cols, part)
            total = total + f32_dot_nt(attn_all[k, j], weight)
        proj[k, 0] = total[:half]
        proj[k, 1] = total[half:]
        exchange.append(push(proj.at[k, other], proj_in.at[k], to_core))

    returns = []

    def give_back(k):
        exchange[k].wait_recv()
        total = (proj[k, core] + proj_in[k]).astype(bf)
        if k:
            ret[k - 1] = total
            returns.append(push(ret.at[k - 1], columns.at[z], to_z[k]))
        else:
            columns[z] = total

    project(0)
    for copy in heads[1]:
        copy.wait_recv()
    project(1)
    for j in range(1, kv_heads):
        heads[2][j].wait_recv()
        heads[3].append(push(attn_all.at[2, j], attn_all.at[3, j], to_z[1]))
    project(2)
    give_back(1)
    give_back(2)
    give_back(0)
    mix_copy.wait_recv()
    mix_copy = send(mix_all.at[zh], to_z[2])
    for copy in heads[3]:
        copy.wait_recv()
    project(3)
    give_back(3)

    for copy in (load_xp, load_xd, load_gain):
        copy.wait()
    rest = pre - half
    first_rows = xp[:half].astype(f32)
    last_rows = jnp.concatenate([xp[half:].astype(f32), xd[...].astype(f32)], axis=0)
    resid = jnp.where(core == 0, first_rows, last_rows)
    mix_copy.wait_recv()
    expert = me // 2
    mix_cols[...] = jnp.concatenate(
        [
            mix_all[a, b, c, d, pl.ds(expert, 1), :]
            for a in range(2)
            for b in range(2)
            for c in range(2)
            for d in range(2)
        ],
        axis=0,
    ).T
    for copy in returns:
        copy.wait_recv()
    added = jnp.concatenate([columns[a].astype(f32) for a in range(4)], axis=1)
    stream = resid + added
    kept_rows[...] = stream
    mean_sq = jnp.mean(stream * stream, axis=-1, keepdims=True)
    normed = (stream * lax.rsqrt(mean_sq + EPS) * gain[...][None, :]).astype(bf)
    r = half // 2
    for p in range(2):
        tok[core, p, z, y, x] = normed[p * r : (p + 1) * r]

    def near(ref, p):
        return ref.at[0, y] if p == 0 else ref.at[1, :, x]

    def far(ref, p):
        return ref.at[0, 1 - y] if p == 0 else ref.at[1, :, 1 - x]

    def plane(k, side):
        return tok.at[side, :, zk[k]]

    own = tok.at[core, :, z, y, x]
    along = [None, None, send(own, to_z[2]), None]
    along[1] = send(own, to_z[1])
    steps = [to_x, to_y]
    second, last = [], []
    over = [[] for _ in range(4)]

    def spread(k):
        blocks = [tok.at[core, p, zk[k], y, x] for p in range(2)]
        second.append([send(blocks[0], to_x), send(blocks[1], to_y)])
        last.append([send(blocks[0], to_y), send(blocks[1], to_x)])

    def relay(k):
        second[k][0].wait_recv()
        last[k].append(send(tok.at[core, 0, zk[k], y, 1 - x], to_y))
        second[k][1].wait_recv()
        last[k].append(send(tok.at[core, 1, zk[k], 1 - y, x], to_x))
        for p in range(2):
            over[k].append(send(near(plane(k, core), p), to_core))

    def finish(k):
        for copy in last[k]:
            copy.wait_recv()
        for p in range(2):
            over[k].append(send(far(plane(k, core), p), to_core))

    back = [None] * 4

    def compute(k):
        for copy in over[k]:
            copy.wait_recv()
        rows_in = tok[:, :, zk[k]].reshape(16 * r, width)
        lane = lax.broadcasted_iota(jnp.int32, (r, mix_cols.shape[1]), 1)
        factors = []
        for side in range(2):
            for p in range(2):
                at = side * half + p * r
                table = mix_cols[at : at + r, :]
                for spot in range(4):
                    chosen = jnp.where(lane == zk[k] * 4 + spot, table, 0.0)
                    factors.append(jnp.sum(chosen, axis=1, keepdims=True))
        factor = jnp.concatenate(factors, axis=0)
        gate = f32_dot(rows_in, gu[0])
        upper = f32_dot(rows_in, gu[1])
        hidden = (upper + 1.0) * gate * jax.nn.sigmoid(1.702 * gate) * factor
        result = f32_dot(hidden.astype(bf), dn[...]).astype(bf)
        part_out[k] = result.reshape(2, 2, 2, 2, r, width)
        theirs, target = part_out.at[k, other], from_core.at[k]
        back[k] = [push(far(theirs, p), far(target, p), to_core) for p in range(2)]
        back[k] += [push(near(theirs, p), near(target, p), to_core) for p in range(2)]

    firsts, seconds, lasts = [None] * 4, [None] * 4, [None] * 4

    def first(k):
        firsts[k] = []
        for p in range(2):
            back[k][p].wait_recv()
            block = far(part_out.at[k, core], p)
            total = block[...].astype(f32) + far(from_core.at[k], p)[...].astype(f32)
            block[...] = total.astype(bf)
            firsts[k].append(push(block, from_first.at[k, p], to_y if p == 0 else to_x))

    def reduce_second(k):
        seconds[k] = []
        for p in range(2):
            back[k][2 + p].wait_recv()
            firsts[k][p].wait_recv()
            total = near(part_out.at[k, core], p)[...].astype(f32)
            total = total + near(from_core.at[k], p)[...].astype(f32)
            total = total + from_first[k, p].astype(f32)
            mid[k, p] = total.astype(bf)
            away = mid.at[k, p, 1 - (x if p == 0 else y)]
            seconds[k].append(push(away, from_second.at[k, p], to_x if p == 0 else to_y))

    def reduce_third(k):
        totals = []
        for p in range(2):
            seconds[k][p].wait_recv()
            kept = mid[k, p, x if p == 0 else y].astype(f32)
            totals.append(kept + from_second[k, p].astype(f32))
        if k:
            for p in range(2):
                to_send[k - 1, p] = totals[p].astype(bf)
            lasts[k] = push(to_send.at[k - 1], from_z.at[k - 1], to_z[k])
        return totals

    spread(0)
    relay(0)
    along[1].wait_recv()
    spread(1)
    finish(0)
    along[2].wait_recv()
    along[3] = send(tok.at[core, :, zk[2], y, x], to_z[1])
    spread(2)
    relay(1)
    load_gu.wait()
    load_dn.wait()
    compute(0)
    finish(1)
    along[3].wait_recv()
    spread(3)
    relay(2)
    compute(1)
    finish(2)
    relay(3)
    first(1)
    compute(2)
    finish(3)
    first(2)
    reduce_second(1)
    compute(3)
    reduce_third(1)
    reduce_second(2)
    first(3)
    first(0)
    reduce_third(2)
    reduce_second(3)
    reduce_second(0)
    reduce_third(3)
    totals = reduce_third(0)
    for k in range(1, 4):
        lasts[k].wait_recv()
    for p in range(2):
        total = kept_rows[p * r : (p + 1) * r, :] + totals[p]
        for k in range(1, 4):
            total = total + from_z[k - 1, p].astype(f32)
        out_ref[p * r : (p + 1) * r, :] = total.astype(bf)
    for copy in sent:
        copy.wait_send()


def fused_path(
    holders,
    x_pre,
    x_dec,
    prefill_query_rows,
    prefill_key_values,
    decode_query_rows,
    decode_key_values,
    cache,
    cache_len,
    sinks,
    o_weight,
    norm_gain,
    expert_ids,
    route_logits,
    w_gate_up,
    w_down,
):
    tokens, topk = expert_ids.shape
    width = x_pre.shape[1]
    inner, columns = o_weight.shape
    hidden = w_down.shape[1]
    half, r = tokens // 2, tokens // 4
    experts = holders // 2
    kv_heads = prefill_key_values.shape[2] // HEAD_SIZE
    lanes = -(-tokens // LANES) * LANES
    bf, f32 = jnp.bfloat16, jnp.float32
    operands = (
        x_pre,
        x_dec,
        prefill_query_rows,
        prefill_key_values,
        decode_query_rows,
        decode_key_values,
        cache,
        cache_len,
        sinks,
        o_weight.T,
        norm_gain,
        expert_ids.T,
        route_logits.T,
        w_gate_up[0],
        w_down[0],
    )
    grid = (4, 2, 2)
    return pl.pallas_call(
        layer_kernel,
        out_shape=jax.ShapeDtypeStruct((half, width), bf),
        in_specs=[pl.BlockSpec(memory_space=pl.ANY)] * len(operands),
        out_specs=pl.BlockSpec(memory_space=pltpu.VMEM),
        scratch_shapes=[
            pltpu.VMEM(x_pre.shape, bf),
            pltpu.VMEM(x_dec.shape, bf),
            pltpu.VMEM(prefill_query_rows.shape, bf),
            pltpu.VMEM(prefill_key_values.shape, bf),
            pltpu.VMEM(decode_query_rows.shape, bf),
            pltpu.VMEM(decode_key_values.shape, bf),
            pltpu.VMEM(cache.shape, bf),
            pltpu.SMEM(cache_len.shape, jnp.int32),
            pltpu.SMEM(sinks.shape, f32),
            pltpu.VMEM(norm_gain.shape, f32),
            pltpu.VMEM((topk, tokens), jnp.int32),
            pltpu.VMEM((topk, tokens), f32),
            pltpu.VMEM((2, width, hidden), bf),
            pltpu.VMEM((hidden, width), bf),
            pltpu.VMEM((2, 2, columns, inner), bf),
            pltpu.VMEM((2, 2, 2, 2, experts, lanes), f32),
            pltpu.VMEM((lanes, holders), f32),
            pltpu.VMEM((4, kv_heads, tokens, inner // kv_heads), bf),
            pltpu.VMEM((4, 2, half, width // 4), f32),
            pltpu.VMEM((4, half, width // 4), f32),
            pltpu.VMEM((3, half, width // 4), bf),
            pltpu.VMEM((4, half, width // 4), bf),
            pltpu.VMEM((half, width), f32),
            pltpu.VMEM((2, 2, *grid, r, width), bf),
            pltpu.VMEM((4, 2, 2, 2, 2, r, width), bf),
            pltpu.VMEM((4, 2, 2, 2, r, width), bf),
            pltpu.VMEM((4, 2, 2, r, width), bf),
            pltpu.VMEM((4, 2, 2, r, width), bf),
            pltpu.VMEM((4, 2, r, width), bf),
            pltpu.VMEM((3, 2, r, width), bf),
            pltpu.VMEM((3, 2, r, width), bf),
            pltpu.SemaphoreType.DMA((128,)),
            pltpu.SemaphoreType.DMA((128,)),
            pltpu.SemaphoreType.DMA((16,)),
        ],
        compiler_params=pltpu.CompilerParams(
            collective_id=0, has_side_effects=True, vmem_limit_bytes=60 * 2**20
        ),
    )(*operands)


def on_device(holders, *args):
    x_pre, x_dec, query_rows, key_values, o_weight = args[0], args[1], args[2], args[3], args[9]
    pre, dec = x_pre.shape[0], x_dec.shape[0]
    tokens, width = pre + dec, x_pre.shape[1]
    gathered = 2 * holders * (tokens * width * 4 + o_weight.size)
    fits = (
        holders == 16
        and tokens == HEAD_SIZE
        and pre % 8 == 0
        and dec == 8
        and tokens // 2 <= pre
        and key_values.shape[2] == LANES
        and query_rows.shape[1] % (4 * LANES) == 0
        and args[6].shape[2] == LANES
        and width % (4 * LANES) == 0
        and o_weight.shape[1] % 32 == 0
        and gathered < 32 * 2**20
    )
    if fits:
        return fused_path(holders, *args)
    return general_path(*args)


def solution(mesh):
    placed = (
        P(("groups", "ep"), None),
        P(("groups", "ep"), None),
        P(("groups", "ep"), "hp"),
        P(None, ("groups", "ep"), "hp"),
        P(("groups", "ep"), "hp"),
        P(None, ("groups", "ep"), "hp"),
        P(None, ("groups", "ep"), None, "hp"),
        P(("groups", "ep")),
        P("hp"),
        P("hp", "ep"),
        P(),
        P(("groups", "ep"), None),
        P(("groups", "ep"), None),
        P("ep", None, None, "hp"),
        P("ep", "hp", None),
    )
    return jax.shard_map(
        functools.partial(on_device, mesh.shape["ep"]),
        mesh=mesh,
        in_specs=placed,
        out_specs=P(("groups", "ep", "hp"), None),
        check_vma=False,
    )
```
